32 devices in a mesh: group: 2 (over y), sample: 16 (over z, x, core).
Axes of the slice: x: 2, y: 2, z: 4, core: 2. Of those that a mesh axis runs over, the one named last changes fastest.
Arguments:
- patches: bfloat16 [16, 256, 588], P('group', 'sample'), parts along dimension 0, may hold values from -6 to 6
- patch_weight: bfloat16 [16, 588, 1280], P('sample'), may hold values from -0.25 to 0.25
- cls_token: bfloat16 [16, 1280], P('sample'), may hold values from -6 to 6
- pos_embed: bfloat16 [16, 257, 1280], P('sample'), may hold values from -3 to 3
- ln1_gain: float32 [16, 1280], P('sample'), may hold values from 0.5 to 1.5
- ln1_bias: float32 [16, 1280], P('sample'), may hold values from -2 to 2
- w_query: bfloat16 [16, 1280, 640], P('sample'), may hold values from -8 to 8
- w_key: bfloat16 [16, 1280, 640], P('sample'), may hold values from -2 to 2
- w_value: bfloat16 [16, 1280, 640], P('sample'), may hold values from -0.15625 to 0.15625
- w_out: bfloat16 [16, 640, 1280], P('sample'), may hold values from -1 to 1
- lnf_gain: float32 [16, 1280], P('sample'), may hold values from 0.5 to 1.5
- lnf_bias: float32 [16, 1280], P('sample'), may hold values from -2 to 2
- head_w: bfloat16 [16, 1280, 1000], P('sample'), may hold values from -0.875 to 0.875
- head_bias: float32 [16, 1000], P('sample'), may hold values from -6 to 290
Outputs:
- predictive: float32 [16, 1000], P('group'), parts along dimension 0
The draws below stay inside these ranges and needn't reach their ends.
There are 2 independent parts, one for each index of `group`. The reference program is written for one: setup_inputs(seed, part) draws one part's arguments, and reference() takes and returns one part's arrays. A program takes and returns all parts, laid end to end along the dimension named above; an argument that names none is the same for every part. Nothing has to cross between parts.
All inputs are finite; a program needn't handle non-finite values.
Results may differ from the reference program's by a relative error of at most 0.0023.
Values may be sent and summed in bfloat16 or wider, within the bound.
A program may use at most 64 MiB of HBM per device.

```python
import math
import jax
import jax.numpy as jnp
from jax import lax

D = 1280
HEADS = 8
HEAD_DIM = 80
PATCH_DIM = 588
PATCHES = 256
CLASSES = 1000
IMAGES = 8
TOKENS = 257
SAMPLES = 16


def key_matrix(key):
    drawn_keys = jax.random.truncated_normal(jax.random.fold_in(key, 7101), -6.0, 6.0, (SAMPLES, D, HEADS * HEAD_DIM), jnp.float32)
    return drawn_keys * D ** (-0.5)


def draw_w_key(key, part):
    return key_matrix(key).astype(jnp.bfloat16)


def draw_w_query(key, part):
    drawn_query = jax.random.truncated_normal(jax.random.fold_in(key, 7102), -6.0, 6.0, (SAMPLES, D, HEADS * HEAD_DIM), jnp.float32) * D ** (-0.5)
    return drawn_query.astype(jnp.bfloat16)


def draw_head_bias(key, part):
    values_drawn = jax.random.truncated_normal(jax.random.fold_in(key, 7201), -6.0, 6.0, (SAMPLES, CLASSES), jnp.float32)
    return values_drawn


def level_of(stream_key, dims, cuts, smallest, high):
    level, own = 1.0, jax.random.fold_in(stream_key, 6)
    for dim, shards_of in cuts:
        heights = jnp.exp(jax.random.uniform(jax.random.fold_in(own, dim), (shards_of,), jnp.float32, smallest / len(cuts), high / len(cuts)))
        level = level * jnp.repeat(heights, dims[dim] // shards_of).reshape([-1 if axis == dim else 1 for axis in range(len(dims))])
    return level


def noise(own_key, shape, scale, most, pieces=(), dtype=jnp.bfloat16):
    drawn = scale * jax.random.normal(own_key, shape, jnp.float32)
    if pieces:
        drawn = drawn * level_of(own_key, shape, pieces, -0.22, 0.18)
    return jnp.clip(drawn, -most, most).astype(dtype)


def setup_inputs(seed: int = 0, part: int = 0) -> dict:
    keys = jax.random.split(jax.random.key(seed), 15)
    part_splits = jax.random.split(jax.random.fold_in(keys[14], part), 15)
    patches = noise(part_splits[0], (IMAGES, PATCHES, PATCH_DIM), 1.0, 6.0, ((1, 16),))
    patch_weight = noise(keys[1], (SAMPLES, PATCH_DIM, D), PATCH_DIM ** -0.5, 0.25, ((0, 16),))
    cls_token = noise(keys[2], (SAMPLES, D), 1.0, 6.0, ((0, 16),))
    pos_embed = noise(keys[3], (SAMPLES, TOKENS, D), 0.5, 3.0, ((0, 16),))
    ln1_gain = jnp.clip(1.0 + 0.1 * jax.random.normal(keys[4], (SAMPLES, D), jnp.float32), 0.5, 1.5)
    ln1_bias = noise(keys[5], (SAMPLES, D), 0.3, 2.0, ((0, 16),), jnp.float32)
    w_query = draw_w_query(jax.random.fold_in(keys[14], 71), part)
    w_key = draw_w_key(jax.random.fold_in(keys[14], 71), part)
    w_value = noise(keys[8], (SAMPLES, D, HEADS * HEAD_DIM), D ** -0.5, 0.15625, ((0, 16),))
    w_out = noise(keys[9], (SAMPLES, HEADS * HEAD_DIM, D), (HEADS * HEAD_DIM // 16) ** -0.5, 1.0, ((0, 16),))
    lnf_gain = jnp.clip(1.0 + 0.1 * jax.random.normal(keys[10], (SAMPLES, D), jnp.float32), 0.5, 1.5)
    lnf_bias = noise(keys[11], (SAMPLES, D), 0.3, 2.0, ((0, 16),), jnp.float32)
    head_w = noise(keys[12], (SAMPLES, D, CLASSES), (D // 25) ** -0.5, 0.875, ((0, 16),))
    head_bias = draw_head_bias(jax.random.fold_in(keys[14], 71), part)
    return dict(patches=patches, patch_weight=patch_weight, cls_token=cls_token, pos_embed=pos_embed, ln1_gain=ln1_gain, ln1_bias=ln1_bias, w_query=w_query, w_key=w_key, w_value=w_value, w_out=w_out, lnf_gain=lnf_gain, lnf_bias=lnf_bias, head_w=head_w, head_bias=head_bias)


epsilon = 1e-06

def layer_norm(values, gain, shift):
    center = values - lax.optimization_barrier(jnp.mean(values, axis=-1, keepdims=True))
    spread = lax.optimization_barrier(jnp.mean(center * center, axis=-1, keepdims=True))
    return center * lax.rsqrt(spread + epsilon) * gain + shift

def one_sample(patches, packed):
    patch_weight, cls_token, pos_embed, ln1_gain, ln1_bias, w_query, w_key, w_value, w_out, lnf_gain, lnf_bias, head_w, head_bias = packed
    width = patch_weight.shape[1]
    image_count = patches.shape[0]
    flat = patches.reshape(-1, patches.shape[2])
    tokens = jnp.dot(flat, patch_weight, preferred_element_type=jnp.float32).reshape(image_count, -1, width)
    tokens = tokens + pos_embed[1:].astype(jnp.float32)[None]
    leading = cls_token.astype(jnp.float32) + pos_embed[0].astype(jnp.float32)
    lead_norm = layer_norm(leading, ln1_gain, ln1_bias).astype(jnp.bfloat16)
    token_norm = layer_norm(tokens, ln1_gain, ln1_bias).astype(jnp.bfloat16)
    all_norm = jnp.concatenate([jnp.broadcast_to(lead_norm[None, None], (image_count, 1, width)), token_norm], axis=1)
    key_rows = jnp.dot(all_norm.reshape(-1, width), w_key, preferred_element_type=jnp.float32).astype(jnp.bfloat16)
    value_rows = jnp.dot(all_norm.reshape(-1, width), w_value, preferred_element_type=jnp.float32).astype(jnp.bfloat16)
    key_rows = key_rows.reshape(image_count, -1, HEADS, HEAD_DIM)
    value_rows = value_rows.reshape(image_count, -1, HEADS, HEAD_DIM)
    query = jnp.dot(lead_norm[None], w_query, preferred_element_type=jnp.float32).astype(jnp.bfloat16)
    query = query.reshape(HEADS, HEAD_DIM)
    scores = jnp.einsum('hd,ithd->iht', query.astype(jnp.float32), key_rows.astype(jnp.float32)) / math.sqrt(HEAD_DIM)
    attention = jax.nn.softmax(scores, axis=-1).astype(jnp.bfloat16)
    mixed = jnp.einsum('iht,ithd->ihd', attention.astype(jnp.float32), value_rows.astype(jnp.float32))
    mixed = mixed.astype(jnp.bfloat16).reshape(image_count, HEADS * HEAD_DIM)
    hidden = leading[None] + jnp.dot(mixed, w_out, preferred_element_type=jnp.float32)
    final = layer_norm(hidden, lnf_gain, lnf_bias).astype(jnp.bfloat16)
    logits = jnp.dot(final, head_w, preferred_element_type=jnp.float32) + head_bias
    return jax.nn.log_softmax(logits, axis=-1)

def reference(patches, patch_weight, cls_token, pos_embed, ln1_gain, ln1_bias, w_query, w_key, w_value, w_out, lnf_gain, lnf_bias, head_w, head_bias):
    packed = (patch_weight, cls_token, pos_embed, ln1_gain, ln1_bias, w_query, w_key, w_value, w_out, lnf_gain, lnf_bias, head_w, head_bias)
    logp = lax.map(lambda single: one_sample(patches, single), packed)
    peak = lax.optimization_barrier(jnp.max(logp, axis=0))
    total = lax.optimization_barrier(jnp.sum(jnp.exp(logp - peak[None]), axis=0))
    return peak + jnp.log(total) - math.log(logp.shape[0])
```

```python
import functools
import math

import jax
import jax.numpy as jnp
from jax import lax
from jax.experimental import pallas as pl
from jax.experimental.pallas import tpu as pltpu
from jax.sharding import PartitionSpec as P

HEAD_DIM = 80


epsilon = 1e-06


def combined_all(part, axis, combine):
    gathered = jax.tree.map(lambda a: lax.all_gather(a, axis), part)

    def take(source):
        return jax.tree.map(lambda a: lax.dynamic_index_in_dim(a, source, 0, False), gathered)

    return lax.fori_loop(
        1, lax.axis_size(axis), lambda source, state: combine(state, take(source)), take(0)
    )


def layer_norm(values, gain, shift):
    center = values - jnp.mean(values, axis=-1, keepdims=True)
    spread = jnp.mean(center * center, axis=-1, keepdims=True)
    return center * lax.rsqrt(spread + epsilon) * gain + shift


def shards(
    patches,
    patch_weight,
    cls_token,
    pos_embed,
    ln1_gain,
    ln1_bias,
    w_query,
    w_key,
    w_value,
    w_out,
    lnf_gain,
    lnf_bias,
    head_w,
    head_bias,
):
    embed_weight = patch_weight[0]
    position = pos_embed[0]
    gain_first = ln1_gain[0]
    bias_first = ln1_bias[0]
    query_weight = w_query[0]
    pair_weight = jnp.concatenate([w_key[0], w_value[0]], axis=1)
    out_weight = w_out[0]
    width = embed_weight.shape[1]
    inner = query_weight.shape[1]
    head_count = inner // HEAD_DIM
    leading = cls_token[0].astype(jnp.float32) + position[0].astype(jnp.float32)
    lead_norm = layer_norm(leading, gain_first, bias_first).astype(jnp.bfloat16)
    lead_pair = jnp.dot(lead_norm[None], pair_weight, preferred_element_type=jnp.float32).astype(
        jnp.bfloat16
    )
    query = jnp.dot(lead_norm[None], query_weight, preferred_element_type=jnp.float32).astype(
        jnp.bfloat16
    )
    query = query.reshape(head_count, HEAD_DIM)
    portion = lax.all_gather(patches, "sample", axis=1, tiled=True)
    image_count = portion.shape[0]
    row_count = portion.shape[1]
    flat = portion.reshape(-1, portion.shape[2])
    tokens = jnp.dot(flat, embed_weight, preferred_element_type=jnp.float32).reshape(
        image_count, row_count, width
    )
    placed = lax.dynamic_slice_in_dim(position, 1, row_count, 0)
    tokens = tokens + placed.astype(jnp.float32)[None]
    normed = layer_norm(tokens, gain_first, bias_first).astype(jnp.bfloat16)
    paired = jnp.dot(normed.reshape(-1, width), pair_weight, preferred_element_type=jnp.float32)
    key_values = paired.astype(jnp.bfloat16).reshape(image_count, row_count, 2 * inner)
    image_count = key_values.shape[0]
    lead_rows = jnp.broadcast_to(lead_pair[None], (image_count, 1, 2 * inner))
    full_rows = jnp.concatenate([lead_rows, key_values], axis=1)
    key_rows = full_rows[:, :, :inner].reshape(image_count, -1, head_count, HEAD_DIM)
    value_rows = full_rows[:, :, inner:].reshape(image_count, -1, head_count, HEAD_DIM)
    scores = jnp.einsum(
        "hd,ithd->iht", query, key_rows, preferred_element_type=jnp.float32
    ) / math.sqrt(HEAD_DIM)
    attention = jax.nn.softmax(scores, axis=-1).astype(jnp.bfloat16)
    mixed = jnp.einsum("iht,ithd->ihd", attention, value_rows, preferred_element_type=jnp.float32)
    mixed = mixed.astype(jnp.bfloat16).reshape(image_count, inner)
    hidden = leading[None] + jnp.dot(mixed, out_weight, preferred_element_type=jnp.float32)
    final = layer_norm(hidden, lnf_gain[0], lnf_bias[0]).astype(jnp.bfloat16)
    logits = jnp.dot(final, head_w[0], preferred_element_type=jnp.float32) + head_bias[0]
    logp = jax.nn.log_softmax(logits, axis=-1)
    count = lax.axis_size("sample")

    def combine(earlier, later):
        highest = jnp.maximum(earlier[0], later[0])
        summed = earlier[1] * jnp.exp(earlier[0] - highest) + later[1] * jnp.exp(later[0] - highest)
        return (highest, summed)

    peak, total = combined_all((logp, jnp.ones_like(logp)), "sample", combine)
    return peak + jnp.log(total) - math.log(count)


MESH = pl.DeviceIdType.MESH
PLANE = 4
BF16_ROWS = 16
LOWEST = -1e30


def flipped(index, turn, bits):
    out = 0
    for bit in range(bits):
        step = 1 << bit
        out = out + step * ((index // step + turn // step) % 2)
    return out


def split_in_two(values):
    high = values.astype(jnp.bfloat16)
    low = (values - high.astype(jnp.float32)).astype(jnp.bfloat16)
    return jnp.concatenate([high, low], axis=0)


def whole_kernel(
    count,
    heads,
    patches,
    cls_token,
    ln1_gain,
    ln1_bias,
    lnf_gain,
    lnf_bias,
    head_bias,
    patch_weight,
    pos_embed,
    w_query,
    w_key,
    w_value,
    w_out,
    head_w,
    out,
    embed,
    position,
    query_w,
    key_w,
    value_w,
    out_w,
    class_w,
    place,
    slots,
    tokens,
    normed,
    probe,
    gathered,
    peak,
    total,
    part,
    from_pair,
    ring,
    result,
    load_sem,
    recv_sem,
    line_sem,
    across_sem,
    pair_sem,
    relay_sem,
    tail_send,
    tail_recv,
    spread_sem,
):
    me = lax.axis_index("sample")
    core = me % 2
    chip = me // 2
    chips = count // 2
    planes = count // PLANE
    bits = planes.bit_length() - 1
    plane = me // PLANE
    spot = me % PLANE
    beside = plane * PLANE + (spot + 2) % PLANE
    twin = me + 1 - 2 * core
    images, rows, depth = patches.shape
    width = embed.shape[1]
    inner = query_w.shape[1]
    head_dim = inner // heads
    pairs = heads * images

    loads = []
    for index, (source, target) in enumerate(
        (
            (pos_embed, position),
            (w_query, query_w),
            (w_key, key_w),
            (patch_weight, embed),
            (w_value, value_w),
            (w_out, out_w),
            (head_w, class_w),
        )
    ):
        load = pltpu.make_async_copy(source.at[0], target, load_sem.at[index])
        load.start()
        loads.append(load)

    barrier = pltpu.get_barrier_semaphore()
    for step in range(1, chips):
        pl.semaphore_signal(
            barrier,
            inc=1,
            device_id={"sample": 2 * ((chip + step) % chips) + core},
            device_id_type=MESH,
        )
    pl.semaphore_signal(barrier, inc=1, device_id={"sample": twin}, device_id_type=MESH)
    pl.semaphore_wait(barrier, chips)

    def send(source, origin, target, sem):
        return pltpu.make_async_remote_copy(
            src_ref=source,
            dst_ref=slots.at[origin],
            send_sem=sem,
            recv_sem=recv_sem.at[origin],
            device_id={"sample": target},
            device_id_type=MESH,
        )

    def along(turn):
        return flipped(plane, turn, bits) * PLANE + spot

    def across(turn):
        return flipped(plane, turn, bits) * PLANE + (spot + 2) % PLANE

    def other(turn):
        return flipped(plane, turn, bits) * PLANE + spot + 1 - 2 * core

    def other_across(turn):
        return flipped(plane, turn, bits) * PLANE + (spot + 2) % PLANE + 1 - 2 * core

    def arrived(origin):
        send(slots.at[origin], origin, twin, relay_sem.at[0]).wait_recv()

    send(patches, me, beside, across_sem.at[0]).start()
    for turn in range(1, planes):
        send(patches, me, along(turn), line_sem.at[turn]).start()
    send(patches, me, twin, pair_sem.at[0]).start()
    slots[me] = patches[...]

    loads[0].wait()
    place[...] = position[...].astype(jnp.float32)[1:]
    leading = cls_token[...].astype(jnp.float32) + position[0:1, :].astype(jnp.float32)
    gain = ln1_gain[...]
    bias = ln1_bias[...]
    lead = jnp.broadcast_to(layer_norm(leading, gain, bias), (BF16_ROWS, width)).astype(jnp.bfloat16)
    loads[1].wait()
    query = jnp.dot(lead, query_w[...], preferred_element_type=jnp.float32)[:1]
    row_head = lax.broadcasted_iota(jnp.int32, (pairs, inner), 0) // images
    column = lax.broadcasted_iota(jnp.int32, (pairs, inner), 1)
    own_head = (column >= row_head * head_dim) & (column < (row_head + 1) * head_dim)
    spread = jnp.where(own_head, jnp.broadcast_to(query, (pairs, inner)), 0.0).astype(jnp.bfloat16)
    loads[2].wait()
    turned = lax.dot_general(
        spread, key_w[...], (((1,), (1,)), ((), ())), preferred_element_type=jnp.float32
    ) * (1.0 / math.sqrt(head_dim))
    probe[...] = split_in_two(turned)
    lead_row = lead[:1].astype(jnp.float32)
    first = jnp.sum(turned * lead_row, axis=1, keepdims=True)
    peak[...] = jnp.broadcast_to(first, peak.shape)
    total[...] = jnp.ones(total.shape, jnp.float32)
    gathered[...] = jnp.broadcast_to(lead_row, gathered.shape)
    loads[3].wait()

    span = PLANE * images * rows
    token_image = (lax.broadcasted_iota(jnp.int32, (pairs, span), 1) // rows) % images
    row_image = lax.broadcasted_iota(jnp.int32, (pairs, span), 0) % images
    same = token_image == row_image

    def turn_step(turn, carry):
        @pl.when(turn < planes)
        def _():
            origin = along(turn)
            arrived(origin)
            send(slots.at[origin], origin, beside, across_sem.at[turn]).start()
            send(slots.at[origin], origin, twin, pair_sem.at[turn]).start()

        done = turn - 1
        origin = across(done)
        arrived(origin)
        send(slots.at[origin], origin, twin, relay_sem.at[done]).start()
        arrived(other(done))
        arrived(other_across(done))

        where = flipped(plane, done, bits)
        block = slots[pl.ds(where * PLANE, PLANE)].reshape(span, depth)
        tokens[...] = jnp.dot(block, embed[...], preferred_element_type=jnp.float32)
        for one in range(PLANE):
            low = one * images * rows
            start = pl.multiple_of((where * PLANE + one) * rows, rows)
            spots = place[pl.ds(start, rows), :]
            value = tokens[low : low + images * rows, :].reshape(images, rows, width) + spots[None]
            value = layer_norm(value, gain[None], bias[None])
            normed[low : low + images * rows, :] = value.reshape(images * rows, width).astype(
                jnp.bfloat16
            )
        scores = lax.dot_general(
            probe[...], normed[...], (((1,), (1,)), ((), ())), preferred_element_type=jnp.float32
        )
        scores = jnp.where(same, scores[:pairs] + scores[pairs:], LOWEST)
        before = peak[:, :1]
        now = jnp.maximum(before, jnp.max(scores, axis=1, keepdims=True))
        shrink = jnp.exp(before - now)
        chance = jnp.where(same, jnp.exp(scores - now), 0.0)
        peak[...] = jnp.broadcast_to(now, peak.shape)
        total[...] = total[...] * shrink + jnp.sum(chance, axis=1, keepdims=True)
        gathered[...] = gathered[...] * shrink + jnp.dot(
            chance.astype(jnp.bfloat16), normed[...], preferred_element_type=jnp.float32
        )
        return carry

    lax.fori_loop(1, planes + 1, turn_step, 0)

    loads[4].wait()
    pooled = gathered[...] / total[:, :1]
    values = jnp.dot(split_in_two(pooled), value_w[...], preferred_element_type=jnp.float32)
    values = jnp.where(own_head, values[:pairs] + values[pairs:], 0.0)
    mixed = jnp.sum(values.reshape(heads, images, inner), axis=0).astype(jnp.bfloat16)
    loads[5].wait()
    hidden = leading + jnp.dot(mixed, out_w[...], preferred_element_type=jnp.float32)
    final = layer_norm(hidden, lnf_gain[...], lnf_bias[...]).astype(jnp.bfloat16)
    loads[6].wait()
    logits = jnp.dot(final, class_w[...], preferred_element_type=jnp.float32) + head_bias[...]
    lifted = logits - jnp.max(logits, axis=-1, keepdims=True)
    logp = lifted - jnp.log(jnp.sum(jnp.exp(lifted), axis=-1, keepdims=True))

    half = part.shape[2]
    classes = out.shape[1]
    part[0] = logp[:, :half]
    part[1] = jnp.concatenate(
        [logp[:, half:], jnp.zeros((images, 2 * half - classes), jnp.float32)], axis=1
    )
    swap = pltpu.make_async_remote_copy(
        src_ref=part.at[1 - core],
        dst_ref=from_pair,
        send_sem=tail_send.at[0],
        recv_sem=tail_recv.at[0],
        device_id={"sample": twin},
        device_id_type=MESH,
    )
    swap.start()
    swap.wait_recv()
    mine = part[core]
    theirs = from_pair[...]
    high = jnp.maximum(mine, theirs)
    ring[chip] = high + jnp.log(jnp.exp(mine - high) + jnp.exp(theirs - high))

    def pass_on(origin, target, step):
        return pltpu.make_async_remote_copy(
            src_ref=ring.at[origin],
            dst_ref=ring.at[origin],
            send_sem=spread_sem.at[step],
            recv_sem=tail_recv.at[2 + origin],
            device_id={"sample": target},
            device_id_type=MESH,
        )

    for step in range(1, chips):
        pass_on(chip, 2 * ((chip + step) % chips) + core, step).start()
    for step in range(1, chips):
        pass_on((chip + step) % chips, me, step).wait_recv()
    every = ring[...]
    high = jnp.max(every, axis=0)
    result[core] = high + jnp.log(jnp.sum(jnp.exp(every - high[None]), axis=0)) - math.log(count)
    share = pltpu.make_async_remote_copy(
        src_ref=result.at[core],
        dst_ref=result.at[core],
        send_sem=tail_send.at[1],
        recv_sem=tail_recv.at[1],
        device_id={"sample": twin},
        device_id_type=MESH,
    )
    share.start()
    for turn in range(planes):
        send(patches, me, beside, across_sem.at[turn]).wait_send()
        send(patches, me, twin, pair_sem.at[turn]).wait_send()
        send(patches, me, twin, relay_sem.at[turn]).wait_send()
        if turn:
            send(patches, me, twin, line_sem.at[turn]).wait_send()
    swap.wait_send()
    for step in range(1, chips):
        pass_on(chip, twin, step).wait_send()
    pltpu.make_async_remote_copy(
        src_ref=result.at[core],
        dst_ref=result.at[1 - core],
        send_sem=tail_send.at[1],
        recv_sem=tail_recv.at[1],
        device_id={"sample": twin},
        device_id_type=MESH,
    ).wait_recv()
    share.wait_send()
    out[:, :half] = result[0]
    out[:, half:] = result[1][:, : classes - half]


def kernel_shards(
    patches,
    patch_weight,
    cls_token,
    pos_embed,
    ln1_gain,
    ln1_bias,
    w_query,
    w_key,
    w_value,
    w_out,
    lnf_gain,
    lnf_bias,
    head_w,
    head_bias,
):
    count = lax.axis_size("sample")
    images, rows, depth = patches.shape
    width = patch_weight.shape[2]
    inner = w_query.shape[2]
    heads = inner // HEAD_DIM
    pairs = heads * images
    planes = count // PLANE
    chips = count // 2
    classes = head_w.shape[2]
    half = pl.cdiv(classes, 256) * 128
    span = PLANE * images * rows
    near = pl.BlockSpec(memory_space=pltpu.VMEM)
    far = pl.BlockSpec(memory_space=pl.ANY)
    dma = pltpu.SemaphoreType.DMA
    f32, bf16 = jnp.float32, jnp.bfloat16
    large = (patch_weight, pos_embed, w_query, w_key, w_value, w_out, head_w)
    embed, position, query_w, key_w, value_w, out_w, class_w = (
        pltpu.VMEM(a.shape[1:], a.dtype) for a in large
    )
    return pl.pallas_call(
        functools.partial(whole_kernel, count, heads),
        out_shape=jax.ShapeDtypeStruct((images, classes), f32),
        in_specs=[near] * 7 + [far] * 7,
        out_specs=near,
        scratch_shapes=[
            embed,
            position,
            query_w,
            key_w,
            value_w,
            out_w,
            class_w,
            pltpu.VMEM((rows * count, width), f32),
            pltpu.VMEM((count, images, rows, depth), bf16),
            pltpu.VMEM((span, width), f32),
            pltpu.VMEM((span, width), bf16),
            pltpu.VMEM((2 * pairs, width), bf16),
            pltpu.VMEM((pairs, width), f32),
            pltpu.VMEM((pairs, 128), f32),
            pltpu.VMEM((pairs, 128), f32),
            pltpu.VMEM((2, images, half), f32),
            pltpu.VMEM((images, half), f32),
            pltpu.VMEM((chips, images, half), f32),
            pltpu.VMEM((2, images, half), f32),
            dma((7,)),
            dma((count,)),
            dma((planes,)),
            dma((planes,)),
            dma((planes,)),
            dma((planes,)),
            dma((2,)),
            dma((2 + chips,)),
            dma((chips,)),
        ],
        compiler_params=pltpu.CompilerParams(
            collective_id=0, has_side_effects=True, vmem_limit_bytes=60 << 20
        ),
    )(patches, cls_token, ln1_gain, ln1_bias, lnf_gain, lnf_bias, head_bias, *large)


def takes_kernel(mesh, patches):
    count = mesh.shape["sample"]
    planes = count // PLANE
    rows = patches.shape[1] // count
    return count % PLANE == 0 and planes & (planes - 1) == 0 and rows % BF16_ROWS == 0


def solution(mesh):
    placed = (
        P("group", "sample", None),
        P("sample", None, None),
        P("sample", None),
        P("sample", None, None),
        P("sample", None),
        P("sample", None),
        P("sample", None, None),
        P("sample", None, None),
        P("sample", None, None),
        P("sample", None, None),
        P("sample", None),
        P("sample", None),
        P("sample", None, None),
        P("sample", None),
    )

    def run(*arrays):
        step = kernel_shards if takes_kernel(mesh, arrays[0]) else shards
        return jax.shard_map(
            step, mesh=mesh, in_specs=placed, out_specs=P("group", None), check_vma=False
        )(*arrays)

    return run
```
